512 devices in a mesh: groups: 2 (over y), seq: 16 (over z), head: 8 (over x), layer: 2 (over core).
Axes of the slice: x: 8, y: 2, z: 16, core: 2. Of those that a mesh axis runs over, the one named last changes fastest.
The devices are a block of a 8x16x16 slice.
Arguments:
- kv_cache: bfloat16 [2, 2, 8, 16384, 8, 128], P(None, 'layer', 'groups', 'seq', 'head'), parts along dimension 2, may hold values from -800 to 800
- valid_blocks: int32 [8], P('groups'), parts along dimension 0, may hold values from 1 to 128, 256 in all
Outputs:
- decode_cache: bfloat16 [2, 2, 32, 4096, 8, 128], P(None, 'layer', ('groups', 'seq'), None, 'head'), parts along dimension 2
- centers: float32 [2, 2, 8, 8, 128], P(None, 'layer', 'groups', 'head'), parts along dimension 2
- scales: float32 [2, 2, 8, 8, 128], P(None, 'layer', 'groups', 'head'), parts along dimension 2
The draws below stay inside these ranges and needn't reach their ends.
There are 2 independent parts, one for each index of `groups`. The reference program is written for one: setup_inputs(seed, part) draws one part's arguments, and reference() takes and returns one part's arrays. A program takes and returns all parts, laid end to end along the dimension named above; each array names one. Nothing has to cross between parts.
Inputs may be any that keep to these rules, and one draw needn't show every extreme that they name: `valid_blocks`: the counts of the 4 users sum to 256, and the largest equals 128.
All inputs are finite; a program needn't handle non-finite values.
Results may differ from the reference program's by a relative error of at most 0.001.
Values may be sent and summed in bfloat16 or wider, within the bound.
No kernel may reach another device: no remote copies, remote signals or barrier semaphores. Data moves between devices by JAX's collectives and lax.ppermute only.
A program may use at most 64 MiB of HBM per device.

```python
import math
import jax
import jax.numpy as jnp
import numpy as np

HEAD = 128
KVH = 8
LAYERS = 2
USERS = 4
PDEV = 1024
BLOCK = 128
SEQ = 16384
NBLK = 128
N_SEQ = 16


def draw_kv_cache(key, part):
    shape = (2, LAYERS, USERS, SEQ, KVH, HEAD)
    row_shape = (2, LAYERS, USERS, SEQ, KVH, 1)
    col_shape = (2, LAYERS, USERS, 1, KVH, HEAD)
    keys = jax.random.split(jax.random.fold_in(key, 11), 4)
    cols = jnp.exp(jax.random.uniform(keys[1], col_shape, jnp.float32, 0.0, math.log(10.0)))
    trend = 1.0 + 2.0 * jnp.arange(SEQ, dtype=jnp.float32).reshape(1, 1, 1, SEQ, 1, 1) / SEQ
    rows = jnp.exp(jax.random.uniform(keys[0], row_shape, jnp.float32, 0.0, math.log(10.0)))
    noise = jnp.clip(jax.random.normal(keys[2], shape, jnp.float32), -4.0, 4.0)
    offset = jnp.clip(jax.random.normal(keys[3], col_shape, jnp.float32), -4.0, 4.0) * 3.0 * cols
    value = trend * (offset + 0.3 * rows * cols * noise)
    return value.astype(jnp.bfloat16)


def split_up(amount, total, reach, skew):
    portions = [(1 << 20) // math.isqrt(standing ** skew) + 1 for standing in range(2, amount + 1)]
    spare, counts = total - reach - (amount - 1), [1] * (amount - 1)
    while spare > 0:
        candidates = [i for i in range(amount - 1) if counts[i] < reach]
        pool, remaining = sum([portions[i] for i in candidates]), spare
        for i in candidates:
            more = min(reach - counts[i], max(1, remaining * portions[i] // pool), spare)
            counts[i] = counts[i] + more
            spare = spare - more
    return np.array([reach] + counts)


def uneven_parts(key, count, total, limit, lean):
    if count == 2:
        one = jax.random.randint(key, (), max(1, total - limit), min(limit, total - 1) + 1)
        return jnp.stack([one, total - one])
    sizes = jnp.asarray(split_up(count, total, limit, lean), jnp.int32)
    pairs = (count - 1) // 2
    donor, sink = sizes[1:1 + 2 * pairs:2], sizes[2:2 + 2 * pairs:2]
    margin = jnp.minimum(donor - 1, limit - sink)
    shifted = jax.random.randint(jax.random.fold_in(key, 1), (pairs,), 0, 1 << 20) % (margin + 1)
    sizes = sizes.at[1:1 + 2 * pairs:2].set(donor - shifted).at[2:2 + 2 * pairs:2].set(sink + shifted)
    return sizes[jax.random.permutation(jax.random.fold_in(key, 2), count)]


def setup_inputs(seed: int = 0, part: int = 0) -> dict:
    key_list = jax.random.split(jax.random.key(seed), 3)
    part_keys = jax.random.split(jax.random.fold_in(key_list[2], part), 3)
    return {
        "kv_cache": draw_kv_cache(jax.random.fold_in(jax.random.fold_in(key_list[2], part), 71), part),
        "valid_blocks": uneven_parts(part_keys[1], USERS, USERS * NBLK // 2, NBLK, 2).astype(jnp.int32),
    }


epsilon = 1e-6


def reference(kv_cache, valid_blocks):
    lengths = valid_blocks.astype(jnp.int32) * BLOCK
    values = kv_cache.astype(jnp.float32)
    position = jnp.arange(SEQ, dtype=jnp.int32)
    is_live = position[None, :] < lengths[:, None]
    live_mask = is_live[None, None, :, :, None, None]
    totals = jnp.sum(jnp.where(live_mask, values, 0.0), axis=3)
    centers = totals / lengths.astype(jnp.float32)[None, None, :, None, None]
    spread = jnp.max(jnp.where(live_mask, jnp.abs(values - centers[:, :, :, None]), 0.0), axis=3)
    scales = spread + epsilon
    normed = jnp.where(live_mask, (values - centers[:, :, :, None]) / scales[:, :, :, None], 0.0).astype(jnp.bfloat16)
    owns = N_SEQ // USERS
    slice_len = PDEV // owns
    shaped = normed.reshape(2, LAYERS, USERS, N_SEQ, owns, slice_len, KVH, HEAD)
    shaped = jnp.transpose(shaped, (0, 1, 2, 4, 3, 5, 6, 7))
    decode_cache = shaped.reshape(2, LAYERS, USERS * owns, N_SEQ * slice_len, KVH, HEAD)
    return decode_cache, centers, scales
```

```python
import functools

import jax
import jax.numpy as jnp
from jax import lax
from jax.experimental import pallas as pl
from jax.experimental.pallas import tpu as pltpu
from jax.sharding import PartitionSpec as P


BLOCK = 128
epsilon = 1e-06
ceiling_value = 3e38


def build_kernel(n, count, info_ref, x_ref, *refs):
    outs, acc = refs[:-1], refs[-1]
    kinds, _, part, head = x_ref.shape
    users = info_ref.shape[0] - 1 - count
    quarter = n // users
    per_dev = quarter * part
    for u in range(users):
        live = jnp.clip(info_ref[u] - info_ref[users], 0, per_dev)
        for k in range(kinds):

            def body(b, carry):
                s, hi, lo = carry
                at = pl.multiple_of(lax.rem(b, part // BLOCK) * BLOCK, BLOCK)
                v = x_ref[k, u * quarter + b // (part // BLOCK), pl.ds(at, BLOCK), :].astype(jnp.float32)
                v = v.reshape(BLOCK // 8, 8, head)
                return s + v.sum(0), jnp.maximum(hi, v.max(0)), jnp.minimum(lo, v.min(0))

            z = jnp.zeros((8, head), jnp.float32)
            s, hi, lo = lax.fori_loop(0, live // BLOCK, body, (z, z - ceiling_value, z + ceiling_value))
            row = k * users + u
            acc[0, row:row + 1, :] = s.sum(0, keepdims=True)
            acc[1, row:row + 1, :] = hi.max(0, keepdims=True)
            acc[2, row:row + 1, :] = lo.min(0, keepdims=True)
    s = acc[0]
    p0 = s.astype(jnp.bfloat16)
    s = s - p0.astype(jnp.float32)
    p1 = s.astype(jnp.bfloat16)
    s = s - p1.astype(jnp.float32)
    p2 = s.astype(jnp.bfloat16)
    tail = jnp.concatenate([p0, p1, p2, acc[1].astype(jnp.bfloat16), acc[2].astype(jnp.bfloat16)], axis=0)
    for j in range(len(outs)):
        to = info_ref[users + 1 + j] if j < count else None

        def fill(at, j=j):
            for k in range(kinds):
                outs[j][k * part:(k + 1) * part, :] = x_ref[k, at]
            outs[j][kinds * part:, :] = tail

        if j < count:
            pl.when(to >= 0)(lambda: fill(to))
    return


def final_kernel(n, count, users, meta_ref, len_ref, *refs):
    slots = refs[:count]
    out_ref, c_ref, s_ref = refs[count], refs[count + 1], refs[count + 2]
    kinds, full, head = out_ref.shape
    part = full // n
    rows = kinds * users
    base = kinds * part
    u, first, length = meta_ref[count], meta_ref[count + 1], meta_ref[count + 2]
    per_dev = meta_ref[count + 3]
    total = jnp.zeros((rows, head), jnp.float32)
    hi = total - ceiling_value
    lo = total + ceiling_value
    for j in range(count):
        ok = meta_ref[j] >= 0
        r = slots[j]
        f = lambda i: r[base + i * rows:base + (i + 1) * rows, :].astype(jnp.float32)
        sj = (f(0) + f(1)) + f(2)
        total = total + jnp.where(ok, sj, 0.0)
        hi = jnp.maximum(hi, jnp.where(ok, f(3), -ceiling_value))
        lo = jnp.minimum(lo, jnp.where(ok, f(4), ceiling_value))
    row = lax.broadcasted_iota(jnp.int32, (rows, head), 0)
    lens = jnp.ones((rows, head), jnp.float32)
    for k in range(kinds):
        for w in range(users):
            lens = jnp.where(row == k * users + w, len_ref[w].astype(jnp.float32), lens)
    c = total / lens
    s = jnp.maximum(hi - c, c - lo) + epsilon
    c_ref[...] = c
    s_ref[...] = s
    cs = [jnp.sum(jnp.where(row == k * users + u, c, 0.0), axis=0, keepdims=True) for k in range(kinds)]
    ss = [jnp.sum(jnp.where(row == k * users + u, s, 0.0), axis=0, keepdims=True) for k in range(kinds)]
    for j in range(count):
        src = meta_ref[j]

        def put(j=j, src=src):
            pos = src * per_dev + first + lax.broadcasted_iota(jnp.int32, (part, head), 0)
            for k in range(kinds):
                v = (slots[j][k * part:(k + 1) * part, :].astype(jnp.float32) - cs[k]) / ss[k]
                v = jnp.where(pos < length, v, 0.0).astype(jnp.bfloat16)
                out_ref[k, pl.ds(pl.multiple_of(src * part, part), part), :] = v

        pl.when(src >= 0)(put)


def build_one(n, info_ref, x_ref, out, acc):
    build_kernel(n, n, info_ref, x_ref, *[out.at[j] for j in range(n)], None, acc)


def final_one(n, users, meta_ref, len_ref, got, *refs):
    final_kernel(n, n, users, meta_ref, len_ref, *[got.at[j] for j in range(n)], *refs)


def on_device(kv_cache, valid_blocks):
    kinds, _, users, per_dev, _, head = kv_cache.shape
    n = lax.axis_size("seq")
    quarter = n // users
    part = per_dev // quarter
    me = lax.axis_index("seq")
    lengths = valid_blocks.astype(jnp.int32) * BLOCK
    to = src = jnp.arange(n, dtype=jnp.int32)
    parts = kv_cache.reshape(kinds, n, part, head)
    tall = kinds * part + 5 * kinds * users
    info = jnp.concatenate([lengths, (me * per_dev)[None], to])
    sent = pl.pallas_call(
        functools.partial(build_one, n),
        out_shape=jax.ShapeDtypeStruct((n, tall, head), jnp.bfloat16),
        in_specs=[pl.BlockSpec(memory_space=pltpu.SMEM), pl.BlockSpec(memory_space=pltpu.VMEM)],
        out_specs=pl.BlockSpec(memory_space=pltpu.VMEM),
        scratch_shapes=[pltpu.VMEM((3, kinds * users, head), jnp.float32)],
    )(info, parts)
    got = [lax.all_to_all(sent, "seq", split_axis=0, concat_axis=0, tiled=True)]
    u, q = me // quarter, lax.rem(me, quarter)
    meta = jnp.concatenate([src, jnp.stack([u, q * part, lengths[u], jnp.int32(per_dev)])])
    out, centers, scales = pl.pallas_call(
        functools.partial(final_one, n, users),
        out_shape=[
            jax.ShapeDtypeStruct((kinds, n * part, head), jnp.bfloat16),
            jax.ShapeDtypeStruct((kinds * users, head), jnp.float32),
            jax.ShapeDtypeStruct((kinds * users, head), jnp.float32),
        ],
        in_specs=[pl.BlockSpec(memory_space=pltpu.SMEM)] * 2 + [pl.BlockSpec(memory_space=pltpu.VMEM)],
        out_specs=[pl.BlockSpec(memory_space=pltpu.VMEM)] * 3,
    )(meta, lengths, *got)
    return (
        out.reshape(kinds, 1, 1, n * part, 1, head),
        centers.reshape(kinds, 1, users, 1, head),
        scales.reshape(kinds, 1, users, 1, head),
    )


def solution(mesh):
    in_specs = (P(None, "layer", "groups", "seq", "head", None), P("groups"))
    out_specs = (
        P(None, "layer", ("groups", "seq"), None, "head", None),
        P(None, "layer", "groups", "head", None),
        P(None, "layer", "groups", "head", None),
    )
    return jax.shard_map(on_device, mesh=mesh, in_specs=in_specs, out_specs=out_specs, check_vma=False)
```

```python
import functools

import jax
import jax.numpy as jnp
from jax import lax
from jax.experimental import pallas as pl
from jax.experimental.pallas import tpu as pltpu
from jax.sharding import PartitionSpec as P

BLOCK = 128
epsilon = 1e-06
ceiling_value = 3e38
LIMIT = 16 << 20


def live_blocks(blocks, src, per_dev):
    return jnp.clip(blocks - src * (per_dev // BLOCK), 0, per_dev // BLOCK)


def build_kernel(vb_ref, x_hbm, slots, acc, sems):
    kinds, users, _, head = x_hbm.shape
    n = slots.shape[0]
    per_dev = x_hbm.shape[2]
    quarter = n // users
    part = per_dev // quarter
    rows = kinds * users
    per = part // BLOCK
    me = lax.axis_index("seq")
    loads = {}
    for u in range(users):
        for k in range(kinds):
            for q in range(quarter):
                c = pltpu.make_async_copy(
                    x_hbm.at[k, u, pl.ds(q * part, part)],
                    slots.at[u * quarter + q, pl.ds(k * part, part)],
                    sems.at[k * users + u, q],
                )
                loads[k, u, q] = c
    alive = {
        (u, q): live_blocks(vb_ref[u], me, per_dev) > q * per for u in range(users) for q in range(quarter)
    }
    for (k, u, q), c in loads.items():
        pl.when(alive[u, q])(c.start)
    for u in range(users):
        live = live_blocks(vb_ref[u], me, per_dev)
        for k in range(kinds):
            for q in range(quarter):
                pl.when(alive[u, q])(loads[k, u, q].wait)

            def body(b, carry):
                s, hi, lo = carry
                at = pl.multiple_of(k * part + lax.rem(b, per) * BLOCK, BLOCK)
                v = slots[u * quarter + b // per, pl.ds(at, BLOCK), :].astype(jnp.float32)
                v = v.reshape(BLOCK // 8, 8, head)
                return s + v.sum(0), jnp.maximum(hi, v.max(0)), jnp.minimum(lo, v.min(0))

            z = jnp.zeros((8, head), jnp.float32)
            s, hi, lo = lax.fori_loop(0, live, body, (z, z - ceiling_value, z + ceiling_value))
            row = k * users + u
            hi = hi.max(0, keepdims=True)
            lo = lo.min(0, keepdims=True)
            count = (live * BLOCK).astype(jnp.float32)
            acc[0, row:row + 1, :] = s.sum(0, keepdims=True) - count * ((hi + lo) * 0.5)
            acc[1, row:row + 1, :] = hi
            acc[2, row:row + 1, :] = lo
    first = acc[0].astype(jnp.bfloat16)
    second = (acc[0] - first.astype(jnp.float32)).astype(jnp.bfloat16)
    tail = jnp.concatenate([first, second, acc[1].astype(jnp.bfloat16), acc[2].astype(jnp.bfloat16)], axis=0)
    for t in range(n):
        slots[t, kinds * part:, :] = tail


def final_kernel(vb_ref, slots, out_hbm, c_ref, s_ref, out_ref, acc, sems):
    kinds, full, head = out_ref.shape
    n = slots.shape[0]
    part = full // n
    users = vb_ref.shape[0]
    quarter = n // users
    per_dev = part * quarter
    rows = kinds * users
    base = kinds * part
    me = lax.axis_index("seq")
    u, q = me // quarter, lax.rem(me, quarter)
    row = lax.broadcasted_iota(jnp.int32, (rows, head), 0)

    def by_row(values):
        out = jnp.zeros((rows, head), jnp.float32)
        for k in range(kinds):
            for w in range(users):
                out = jnp.where(row == k * users + w, values[w].astype(jnp.float32), out)
        return out

    def read(src, i):
        return slots[src, base + i * rows:base + (i + 1) * rows, :].astype(jnp.float32)

    blocks = by_row([vb_ref[w] for w in range(users)])
    total = jnp.zeros((rows, head), jnp.float32)
    hi, lo = total - ceiling_value, total + ceiling_value
    for src in range(n):
        count = jnp.clip(blocks - src * (per_dev // BLOCK), 0, per_dev // BLOCK) * BLOCK
        top, bottom = read(src, 2), read(src, 3)
        total = total + ((read(src, 0) + read(src, 1)) + count * ((top + bottom) * 0.5))
        hi = jnp.maximum(hi, top)
        lo = jnp.minimum(lo, bottom)
    c = total / (blocks * BLOCK)
    s = jnp.maximum(hi - c, c - lo) + epsilon
    c_ref[...] = c
    s_ref[...] = s
    acc[0] = c
    acc[1] = s
    cs = [acc[0, pl.ds(k * users + u, 1), :] for k in range(kinds)]
    ss = [acc[1, pl.ds(k * users + u, 1), :] for k in range(kinds)]
    blocks_here = vb_ref[u]

    def copy(k, src):
        at = pl.ds(pl.multiple_of(src * part, part), part)
        return pltpu.make_async_copy(out_ref.at[k, at], out_hbm.at[k, at], sems.at[k])

    def one(src, _):
        for b in range(part // BLOCK):
            live = src * (per_dev // BLOCK) + q * (part // BLOCK) + b < blocks_here
            at = pl.multiple_of(src * part + b * BLOCK, BLOCK)

            @pl.when(live)
            def _():
                for k in range(kinds):
                    v = slots[src, k * part + b * BLOCK:k * part + (b + 1) * BLOCK, :].astype(jnp.float32)
                    out_ref[k, pl.ds(at, BLOCK), :] = ((v - cs[k]) / ss[k]).astype(jnp.bfloat16)

            @pl.when(jnp.logical_not(live))
            def _():
                for k in range(kinds):
                    out_ref[k, pl.ds(at, BLOCK), :] = jnp.zeros((BLOCK, head), jnp.bfloat16)

        for k in range(kinds):
            copy(k, src).start()
        return 0

    lax.fori_loop(0, n, one, 0)
    for k in range(kinds):
        pltpu.make_async_copy(out_ref.at[k], out_hbm.at[k], sems.at[k]).wait()


def on_device(kv_cache, valid_blocks):
    kinds, _, users, per_dev, _, head = kv_cache.shape
    n = lax.axis_size("seq")
    part = per_dev * users // n
    rows = kinds * users
    full = n * part
    x = kv_cache.reshape(kinds, users, per_dev, head)
    tall = kinds * part + 4 * rows
    anys = pl.BlockSpec(memory_space=pl.ANY)
    vmem = pl.BlockSpec(memory_space=pltpu.VMEM)
    smem = pl.BlockSpec(memory_space=pltpu.SMEM)
    slots = pl.pallas_call(
        build_kernel,
        out_shape=pltpu.VMEM((n, tall, head), jnp.bfloat16),
        in_specs=[smem, anys],
        out_specs=vmem,
        scratch_shapes=[
            pltpu.VMEM((3, rows, head), jnp.float32),
            pltpu.SemaphoreType.DMA((rows, n // users)),
        ],
    )(valid_blocks, x)
    slots = lax.all_to_all(slots, "seq", split_axis=0, concat_axis=0, tiled=True)
    slots = pltpu.with_memory_space_constraint(slots, pltpu.VMEM)
    small = jax.ShapeDtypeStruct((rows, head), jnp.float32)
    out, centers, scales = pl.pallas_call(
        final_kernel,
        out_shape=[jax.ShapeDtypeStruct((kinds, full, head), jnp.bfloat16), small, small],
        in_specs=[smem, vmem],
        out_specs=[anys, vmem, vmem],
        scratch_shapes=[
            pltpu.VMEM((kinds, full, head), jnp.bfloat16),
            pltpu.VMEM((2, rows, head), jnp.float32),
            pltpu.SemaphoreType.DMA((kinds,)),
        ],
        compiler_params=pltpu.CompilerParams(vmem_limit_bytes=LIMIT),
    )(valid_blocks, slots)
    return (
        out.reshape(kinds, 1, 1, full, 1, head),
        centers.reshape(kinds, 1, users, 1, head),
        scales.reshape(kinds, 1, users, 1, head),
    )


def solution(mesh):
    in_specs = (P(None, "layer", "groups", "seq", "head", None), P("groups"))
    out_specs = (
        P(None, "layer", ("groups", "seq"), None, "head", None),
        P(None, "layer", "groups", "head", None),
        P(None, "layer", "groups", "head", None),
    )
    return jax.shard_map(on_device, mesh=mesh, in_specs=in_specs, out_specs=out_specs, check_vma=False)
```

```python
import functools

import jax
import jax.numpy as jnp
from jax import lax
from jax.experimental import pallas as pl
from jax.experimental.pallas import tpu as pltpu
from jax.sharding import PartitionSpec as P


BLOCK = 128
epsilon = 1e-06
ceiling_value = 3e38
LIMIT = 16 << 20


def shifts(n):
    return [n // 2] + [s * k for k in range(n // 2 - 1, 0, -1) for s in (1, -1)]


def live_blocks(blocks, src, per_dev):
    return jnp.clip(blocks - src * (per_dev // BLOCK), 0, per_dev // BLOCK)


def build_kernel(order, vb_ref, x_hbm, *refs):
    n = len(order) + 1
    slots, (x_ref, acc, in_sems) = refs[:n], refs[n:]
    kinds, users, per_dev, head = x_hbm.shape
    quarter = n // users
    part = per_dev // quarter
    me = lax.axis_index("seq")
    live = [live_blocks(vb_ref[u], me, per_dev) for u in range(users)]
    loads = {
        (k, u): pltpu.make_async_copy(x_hbm.at[k, u], x_ref.at[k, u], in_sems.at[k, u])
        for u in range(users) for k in range(kinds)
    }
    for (k, u), c in loads.items():
        pl.when(live[u] > 0)(c.start)
    for u in range(users):
        for k in range(kinds):
            pl.when(live[u] > 0)(loads[k, u].wait)

            def body(b, carry):
                s, hi, lo = carry
                v = x_ref[k, u, pl.ds(pl.multiple_of(b * BLOCK, BLOCK), BLOCK), :].astype(jnp.float32)
                v = v.reshape(BLOCK // 8, 8, head)
                return s + v.sum(0), jnp.maximum(hi, v.max(0)), jnp.minimum(lo, v.min(0))

            z = jnp.zeros((8, head), jnp.float32)
            s, hi, lo = lax.fori_loop(0, live[u], body, (z, z - ceiling_value, z + ceiling_value))
            row = k * users + u
            hi = hi.max(0, keepdims=True)
            lo = lo.min(0, keepdims=True)
            count = (live[u] * BLOCK).astype(jnp.float32)
            acc[0, row:row + 1, :] = s.sum(0, keepdims=True) - count * ((hi + lo) * 0.5)
            acc[1, row:row + 1, :] = hi
            acc[2, row:row + 1, :] = lo
    first = acc[0].astype(jnp.bfloat16)
    second = (acc[0] - first.astype(jnp.float32)).astype(jnp.bfloat16)
    tail = jnp.concatenate([first, second, acc[1].astype(jnp.bfloat16), acc[2].astype(jnp.bfloat16)], axis=0)
    for j, shift in enumerate(list(order) + [0]):
        to = lax.rem(me + shift + n, n)
        u, q = to // quarter, lax.rem(to, quarter)
        for k in range(kinds):
            slots[j][k * part:(k + 1) * part, :] = x_ref[k, u, pl.ds(pl.multiple_of(q * part, part), part), :]
        slots[j][kinds * part:, :] = tail


def final_kernel(order, vb_ref, *refs):
    n = len(order) + 1
    slots, (out_hbm, c_ref, s_ref, out_ref, acc, sems) = refs[:n], refs[n:]
    kinds, full, head = out_ref.shape
    part = full // n
    users = vb_ref.shape[0]
    quarter = n // users
    per_dev = part * quarter
    rows = kinds * users
    base = kinds * part
    me = lax.axis_index("seq")
    u, q = me // quarter, lax.rem(me, quarter)
    row = lax.broadcasted_iota(jnp.int32, (rows, head), 0)
    blocks = jnp.zeros((rows, head), jnp.float32)
    for k in range(kinds):
        for w in range(users):
            blocks = jnp.where(row == k * users + w, vb_ref[w].astype(jnp.float32), blocks)
    source = [lax.rem(me - shift + n, n) for shift in list(order) + [0]]
    for j in range(n):
        acc[source[j]] = slots[j][base:, :].astype(jnp.float32)
    total = jnp.zeros((rows, head), jnp.float32)
    hi, lo = total - ceiling_value, total + ceiling_value
    for src in range(n):
        a, b, top, bottom = (acc[src, i * rows:(i + 1) * rows, :] for i in range(4))
        count = jnp.clip(blocks - src * (per_dev // BLOCK), 0, per_dev // BLOCK) * BLOCK
        total = total + ((a + b) + count * ((top + bottom) * 0.5))
        hi = jnp.maximum(hi, top)
        lo = jnp.minimum(lo, bottom)
    c = total / (blocks * BLOCK)
    s = jnp.maximum(hi - c, c - lo) + epsilon
    c_ref[...] = c
    s_ref[...] = s
    cs = [c_ref[pl.ds(k * users + u, 1), :] for k in range(kinds)]
    ss = [s_ref[pl.ds(k * users + u, 1), :] for k in range(kinds)]
    blocks_here = vb_ref[u]
    for j in range(n):
        src = source[j]
        for b in range(part // BLOCK):
            live = src * (per_dev // BLOCK) + q * (part // BLOCK) + b < blocks_here
            at = pl.multiple_of(src * part + b * BLOCK, BLOCK)

            @pl.when(live)
            def _():
                for k in range(kinds):
                    v = slots[j][k * part + b * BLOCK:k * part + (b + 1) * BLOCK, :].astype(jnp.float32)
                    out_ref[k, pl.ds(at, BLOCK), :] = ((v - cs[k]) / ss[k]).astype(jnp.bfloat16)

            @pl.when(jnp.logical_not(live))
            def _():
                for k in range(kinds):
                    out_ref[k, pl.ds(at, BLOCK), :] = jnp.zeros((BLOCK, head), jnp.bfloat16)

        for k in range(kinds):
            at = pl.ds(pl.multiple_of(src * part, part), part)
            pltpu.make_async_copy(out_ref.at[k, at], out_hbm.at[k, at], sems.at[k]).start()
    for k in range(kinds):
        pltpu.make_async_copy(out_ref.at[k], out_hbm.at[k], sems.at[k]).wait()


def on_device(kv_cache, valid_blocks):
    kinds, _, users, per_dev, _, head = kv_cache.shape
    n = lax.axis_size("seq")
    part = per_dev * users // n
    rows = kinds * users
    full = n * part
    order = shifts(n)
    x = kv_cache.reshape(kinds, users, per_dev, head)
    tall = kinds * part + 4 * rows
    anys = pl.BlockSpec(memory_space=pl.ANY)
    vmem = pl.BlockSpec(memory_space=pltpu.VMEM)
    smem = pl.BlockSpec(memory_space=pltpu.SMEM)
    slots = pl.pallas_call(
        functools.partial(build_kernel, order),
        out_shape=[pltpu.VMEM((tall, head), jnp.bfloat16)] * n,
        in_specs=[smem, anys],
        out_specs=[vmem] * n,
        scratch_shapes=[
            pltpu.VMEM((kinds, users, per_dev, head), jnp.bfloat16),
            pltpu.VMEM((3, rows, head), jnp.float32),
            pltpu.SemaphoreType.DMA((kinds, users)),
        ],
    )(valid_blocks, x)
    got = []
    for j, shift in enumerate(order):
        got.append(lax.ppermute(slots[j], "seq", [(s, (s + shift) % n) for s in range(n)]))
    got.append(slots[-1])
    got = [pltpu.with_memory_space_constraint(g, pltpu.VMEM) for g in got]
    small = jax.ShapeDtypeStruct((rows, head), jnp.float32)
    out, centers, scales = pl.pallas_call(
        functools.partial(final_kernel, order),
        out_shape=[jax.ShapeDtypeStruct((kinds, full, head), jnp.bfloat16), small, small],
        in_specs=[smem] + [vmem] * n,
        out_specs=[anys, vmem, vmem],
        scratch_shapes=[
            pltpu.VMEM((kinds, full, head), jnp.bfloat16),
            pltpu.VMEM((n, 4 * rows, head), jnp.float32),
            pltpu.SemaphoreType.DMA((kinds,)),
        ],
        compiler_params=pltpu.CompilerParams(vmem_limit_bytes=LIMIT),
    )(valid_blocks, *got)
    return (
        out.reshape(kinds, 1, 1, full, 1, head),
        centers.reshape(kinds, 1, users, 1, head),
        scales.reshape(kinds, 1, users, 1, head),
    )


def solution(mesh):
    in_specs = (P(None, "layer", "groups", "seq", "head", None), P("groups"))
    out_specs = (
        P(None, "layer", ("groups", "seq"), None, "head", None),
        P(None, "layer", "groups", "head", None),
        P(None, "layer", "groups", "head", None),
    )
    return jax.shard_map(on_device, mesh=mesh, in_specs=in_specs, out_specs=out_specs, check_vma=False)
```

```python
import functools

import jax
import jax.numpy as jnp
from jax import lax
from jax.experimental import pallas as pl
from jax.experimental.pallas import tpu as pltpu
from jax.sharding import PartitionSpec as P


BLOCK = 128
epsilon = 1e-06
ceiling_value = 3e38
PIECES = 2
LIMIT = 16 << 20


def shifts(n):
    pairs = [(k, -k) if k % 2 else (-k, k) for k in range(n // 2 - 1, 0, -1)]
    return [n // 2] + [k for pair in pairs for k in pair]


def live_blocks(blocks, src, per_dev):
    return jnp.clip(blocks - src * (per_dev // BLOCK), 0, per_dev // BLOCK)


def build_kernel(order, vb_ref, x_hbm, *refs):
    n = len(order) + 1
    slots, (x_ref, acc, in_sems) = refs[:n], refs[n:]
    kinds, users, per_dev, head = x_hbm.shape
    quarter = n // users
    part = per_dev // quarter
    me = lax.axis_index("seq")
    live = [live_blocks(vb_ref[u], me, per_dev) for u in range(users)]
    loads = {
        (k, u): pltpu.make_async_copy(x_hbm.at[k, u], x_ref.at[k, u], in_sems.at[k, u])
        for u in range(users) for k in range(kinds)
    }
    for (k, u), c in loads.items():
        pl.when(live[u] > 0)(c.start)
    for u in range(users):
        for k in range(kinds):
            pl.when(live[u] > 0)(loads[k, u].wait)

            def body(b, carry):
                s, hi, lo = carry
                v = x_ref[k, u, pl.ds(pl.multiple_of(b * BLOCK, BLOCK), BLOCK), :].astype(jnp.float32)
                v = v.reshape(BLOCK // 8, 8, head)
                return s + v.sum(0), jnp.maximum(hi, v.max(0)), jnp.minimum(lo, v.min(0))

            z = jnp.zeros((8, head), jnp.float32)
            s, hi, lo = lax.fori_loop(0, live[u], body, (z, z - ceiling_value, z + ceiling_value))
            row = k * users + u
            acc[0, row:row + 1, :] = s.sum(0, keepdims=True)
            acc[1, row:row + 1, :] = hi.max(0, keepdims=True)
            acc[2, row:row + 1, :] = lo.min(0, keepdims=True)
    rest, pieces = acc[0], []
    for _ in range(PIECES):
        pieces.append(rest.astype(jnp.bfloat16))
        rest = rest - pieces[-1].astype(jnp.float32)
    tail = jnp.concatenate(pieces + [acc[i].astype(jnp.bfloat16) for i in (1, 2)], axis=0)
    for j, shift in enumerate(list(order) + [0]):
        to = lax.rem(me + shift + n, n)
        u, q = to // quarter, lax.rem(to, quarter)

        @pl.when(live_blocks(vb_ref[u], me, per_dev) > q * (part // BLOCK))
        def _():
            for k in range(kinds):
                slots[j][k * part:(k + 1) * part, :] = x_ref[k, u, pl.ds(pl.multiple_of(q * part, part), part), :]

        slots[j][kinds * part:, :] = tail


def final_kernel(order, vb_ref, *refs):
    n = len(order) + 1
    slots, (out_hbm, c_ref, s_ref, out_ref, acc, sems) = refs[:n], refs[n:]
    kinds, full, head = out_ref.shape
    part = full // n
    users = vb_ref.shape[0]
    quarter = n // users
    per_dev = part * quarter
    rows = kinds * users
    base = kinds * part
    me = lax.axis_index("seq")
    u, q = me // quarter, lax.rem(me, quarter)
    row = lax.broadcasted_iota(jnp.int32, (rows, head), 0)
    blocks = jnp.zeros((rows, head), jnp.float32)
    for k in range(kinds):
        for w in range(users):
            blocks = jnp.where(row == k * users + w, vb_ref[w].astype(jnp.float32), blocks)
    source = [lax.rem(me - shift + n, n) for shift in list(order) + [0]]
    for j in range(n):
        acc[source[j]] = slots[j][base:, :].astype(jnp.float32)
    total = jnp.zeros((rows, head), jnp.float32)
    hi, lo = total - ceiling_value, total + ceiling_value
    for src in range(n):
        *pieces, top, bottom = (acc[src, i * rows:(i + 1) * rows, :] for i in range(PIECES + 2))
        total = total + functools.reduce(jnp.add, pieces)
        hi = jnp.maximum(hi, top)
        lo = jnp.minimum(lo, bottom)
    c = total / (blocks * BLOCK)
    s = jnp.maximum(hi - c, c - lo) + epsilon
    c_ref[...] = c
    s_ref[...] = s
    cs = [c_ref[pl.ds(k * users + u, 1), :] for k in range(kinds)]
    ss = [1.0 / s_ref[pl.ds(k * users + u, 1), :] for k in range(kinds)]
    blocks_here = vb_ref[u]
    for j in range(n):
        src = source[j]
        for b in range(part // BLOCK):
            live = src * (per_dev // BLOCK) + q * (part // BLOCK) + b < blocks_here
            at = pl.multiple_of(src * part + b * BLOCK, BLOCK)

            @pl.when(live)
            def _():
                for k in range(kinds):
                    v = slots[j][k * part + b * BLOCK:k * part + (b + 1) * BLOCK, :].astype(jnp.float32)
                    out_ref[k, pl.ds(at, BLOCK), :] = ((v - cs[k]) * ss[k]).astype(jnp.bfloat16)

            @pl.when(jnp.logical_not(live))
            def _():
                for k in range(kinds):
                    out_ref[k, pl.ds(at, BLOCK), :] = jnp.zeros((BLOCK, head), jnp.bfloat16)

        for k in range(kinds):
            at = pl.ds(pl.multiple_of(src * part, part), part)
            pltpu.make_async_copy(out_ref.at[k, at], out_hbm.at[k, at], sems.at[k]).start()
    for k in range(kinds):
        pltpu.make_async_copy(out_ref.at[k], out_hbm.at[k], sems.at[k]).wait()


def on_device(kv_cache, valid_blocks):
    kinds, _, users, per_dev, _, head = kv_cache.shape
    n = lax.axis_size("seq")
    part = per_dev * users // n
    rows = kinds * users
    full = n * part
    order = shifts(n)
    x = kv_cache.reshape(kinds, users, per_dev, head)
    tall = kinds * part + (PIECES + 2) * rows
    anys = pl.BlockSpec(memory_space=pl.ANY)
    vmem = pl.BlockSpec(memory_space=pltpu.VMEM)
    smem = pl.BlockSpec(memory_space=pltpu.SMEM)
    slots = pl.pallas_call(
        functools.partial(build_kernel, order),
        out_shape=[pltpu.VMEM((tall, head), jnp.bfloat16)] * n,
        in_specs=[smem, anys],
        out_specs=[vmem] * n,
        scratch_shapes=[
            pltpu.VMEM((kinds, users, per_dev, head), jnp.bfloat16),
            pltpu.VMEM((3, rows, head), jnp.float32),
            pltpu.SemaphoreType.DMA((kinds, users)),
        ],
    )(valid_blocks, x)
    got = []
    for j, shift in enumerate(order):
        got.append(lax.ppermute(slots[j], "seq", [(s, (s + shift) % n) for s in range(n)]))
    got.append(slots[-1])
    got = [pltpu.with_memory_space_constraint(g, pltpu.VMEM) for g in got]
    small = jax.ShapeDtypeStruct((rows, head), jnp.float32)
    out, centers, scales = pl.pallas_call(
        functools.partial(final_kernel, order),
        out_shape=[jax.ShapeDtypeStruct((kinds, full, head), jnp.bfloat16), small, small],
        in_specs=[smem] + [vmem] * n,
        out_specs=[anys, vmem, vmem],
        scratch_shapes=[
            pltpu.VMEM((kinds, full, head), jnp.bfloat16),
            pltpu.VMEM((n, (PIECES + 2) * rows, head), jnp.float32),
            pltpu.SemaphoreType.DMA((kinds,)),
        ],
        compiler_params=pltpu.CompilerParams(vmem_limit_bytes=LIMIT),
    )(valid_blocks, *got)
    return (
        out.reshape(kinds, 1, 1, full, 1, head),
        centers.reshape(kinds, 1, users, 1, head),
        scales.reshape(kinds, 1, users, 1, head),
    )


def solution(mesh):
    in_specs = (P(None, "layer", "groups", "seq", "head", None), P("groups"))
    out_specs = (
        P(None, "layer", ("groups", "seq"), None, "head", None),
        P(None, "layer", "groups", "head", None),
        P(None, "layer", "groups", "head", None),
    )
    return jax.shard_map(on_device, mesh=mesh, in_specs=in_specs, out_specs=out_specs, check_vma=False)
```
